32 devices in a mesh: replica: 1 (over z), data2: 4 (over y), data: 8 (over x, core).
Axes of the slice: x: 4, y: 4, z: 1, core: 2. Of those that a mesh axis runs over, the one named last changes fastest.
The devices are a block of a 4x4x8 slice.
Arguments:
- query_hidden: bfloat16 [128, 32, 2048], P(('replica', 'data2', 'data'))
- doc_hidden: bfloat16 [128, 768, 2048], P(('replica', 'data2', 'data'))
- w_proj: bfloat16 [2048, 128], replicated
- query_mask: int32 [128, 32], P(('replica', 'data2', 'data'))
- doc_mask: int32 [128, 768], P(('replica', 'data2', 'data'))
- temperature: float32 [], replicated
Outputs:
- output 1: float32 [128], P(('replica', 'data2', 'data'))
- output 2: float32 [1], P('replica')
All inputs are finite; a program needn't handle non-finite values.
Results may differ from the reference program's by a relative error of at most 0.001.
Values are sent between devices in bfloat16 or wider.
A program may use at most 768 MiB of HBM per device.

```python
import jax
import jax.numpy as jnp
from jax import lax

BATCH = 128
QLEN = 32
DLEN = 768
HIDDEN = 2048
PROJ = 128


def setup_inputs(seed: int = 0, part: int = 0) -> dict:
    root_key = jax.random.key(seed)
    key_common, key_parts = jax.random.split(root_key)
    part_key = jax.random.fold_in(key_parts, part)
    key_list = jax.random.split(part_key, 6)
    key_weight, key_temp = jax.random.split(key_common)
    shared = jax.random.normal(key_list[0], (HIDDEN,), jnp.float32)
    topic_vec = jax.random.normal(key_list[1], (BATCH, 1, HIDDEN), jnp.float32)
    concept = jax.random.normal(key_list[2], (BATCH, QLEN, HIDDEN), jnp.float32)
    token_noise = jax.random.normal(key_list[3], (BATCH, DLEN, HIDDEN), jnp.float32)
    query_lens = jax.random.randint(key_list[4], (BATCH,), QLEN // 2, QLEN + 1)
    doc_lens = jax.random.randint(key_list[5], (BATCH,), DLEN // 4, DLEN + 1)
    query_mask = (jnp.arange(QLEN)[None, :] < query_lens[:, None]).astype(jnp.int32)
    doc_mask = (jnp.arange(DLEN)[None, :] < doc_lens[:, None]).astype(jnp.int32)
    base_state = 0.6 * shared + 0.6 * topic_vec
    query_hidden = base_state + concept
    doc_concept = jnp.take(concept, jnp.arange(DLEN) % QLEN, axis=1)
    real_tok = base_state + 0.6 * doc_concept + 0.8 * token_noise
    pad_tok = 1.5 * shared + token_noise
    doc_hidden = jnp.where(doc_mask[:, :, None] > 0, real_tok, pad_tok)
    w_proj = jax.random.normal(key_weight, (HIDDEN, PROJ), jnp.float32) * HIDDEN ** -0.5
    temperature = QLEN * jax.random.uniform(key_temp, (), jnp.float32, 0.8, 1.25) / 8.0
    return {'query_hidden': query_hidden.astype(jnp.bfloat16), 'doc_hidden': doc_hidden.astype(jnp.bfloat16), 'w_proj': w_proj.astype(jnp.bfloat16), 'query_mask': query_mask, 'doc_mask': doc_mask, 'temperature': temperature}


def project_norm(hidden, w_proj):
    flat_states = hidden.reshape(-1, HIDDEN)
    projected = jnp.dot(flat_states, w_proj, preferred_element_type=jnp.float32)
    norm_len = jnp.sqrt(jnp.sum(projected * projected, axis=-1, keepdims=True))
    unit_vecs = projected / jnp.maximum(norm_len, 1e-12)
    return unit_vecs.astype(jnp.bfloat16).reshape(hidden.shape[0], hidden.shape[1], PROJ)


def reference(query_hidden, doc_hidden, w_proj, query_mask, doc_mask, temperature):
    q_vecs = project_norm(query_hidden, w_proj)
    p_vecs = project_norm(doc_hidden, w_proj).astype(jnp.float32)
    doc_valid = doc_mask[None, :, :] > 0

    def query_row(query_args):
        q_tok, q_weight = query_args
        similarity = jnp.einsum('tc,jsc->tjs', q_tok.astype(jnp.float32), p_vecs)
        best_match = jnp.max(jnp.where(doc_valid, similarity, -jnp.inf), axis=-1)
        return jnp.sum(q_weight.astype(jnp.float32)[:, None] * best_match, axis=0)

    scores = lax.map(query_row, (q_vecs, query_mask))
    logits = scores / temperature
    losses = jax.nn.logsumexp(logits, axis=1) - jnp.diagonal(logits)
    mean_loss = jnp.mean(losses).reshape(1)
    return losses, mean_loss
```

```python
import functools

import jax
import jax.numpy as jnp
from jax import lax
from jax.experimental import pallas as pl
from jax.experimental.pallas import tpu as pltpu
from jax.sharding import PartitionSpec as P

MESH = pl.DeviceIdType.MESH
F32 = jnp.float32
BF16 = jnp.bfloat16
CORES = 2


def chip_order(ny, nx):
    def hops(d, n):
        return min(d, n - d)
    return sorted(
        ((dy, dx) for dy in range(ny) for dx in range(nx)),
        key=lambda o: (hops(o[0], ny) + hops(o[1], nx), max(hops(o[0], ny), hops(o[1], nx)), o),
    )


def kernel(cfg, q_hbm, d_hbm, w_hbm, qm_hbm, dm_hbm, temp_hbm, loss_ref, mean_ref,
           qbuf, dbuf, wbuf, qmbuf, dmbuf, dm8, tbuf, qt_all, p_buf, mcol, s_all,
           insem, dsem, qsend, qrecv, fsend, frecv, ssend, srecv):
    ny, nx, nq, qlen, ndoc, dlen, chunk, rows = cfg
    nchip = ny * nx
    ndev = nchip * CORES
    proj = w_hbm.shape[1]
    lanes = nq * qlen
    nchunk = ndoc * dlen // chunk
    per_doc = dlen // chunk
    group = 2
    order = chip_order(ny, nx)

    y = lax.axis_index("data2")
    dx_ = lax.axis_index("data")
    x = dx_ // CORES
    core = dx_ % CORES
    chip = y * nx + x
    me = chip * CORES + core
    other = 1 - core

    def rel(k):
        oy, ox = order[k]
        cy = lax.rem(y + oy, ny)
        cx = lax.rem(x + ox, nx)
        return cy, cx, cy * nx + cx

    def dev(cy, cx, c):
        return {"data2": cy, "data": cx * CORES + c}

    copies = [
        pltpu.make_async_copy(q_hbm, qbuf, insem.at[0]),
        pltpu.make_async_copy(w_hbm, wbuf, insem.at[1]),
        pltpu.make_async_copy(qm_hbm, qmbuf, insem.at[2]),
        pltpu.make_async_copy(dm_hbm, dmbuf, insem.at[3]),
        pltpu.make_async_copy(temp_hbm, tbuf, insem.at[4]),
    ]
    for cp in copies:
        cp.start()

    def doc_copy(c):
        part = pl.ds(c * chunk, chunk)
        return pltpu.make_async_copy(d_hbm.at[part], dbuf.at[part], dsem.at[c])

    for c in range(nchunk):
        doc_copy(c).start()

    barrier = pltpu.get_barrier_semaphore()
    for k in range(nchip):
        cy, cx, _ = rel(k)
        for c in range(CORES):
            tgt = core if c == 0 else other
            if k == 0 and c == 0:
                continue
            pl.semaphore_signal(barrier, inc=1, device_id=dev(cy, cx, tgt), device_id_type=MESH)

    copies[2].wait()
    lane = lax.broadcasted_iota(jnp.int32, (8, lanes), 1)
    sub = lax.broadcasted_iota(jnp.int32, (8, lanes), 0)
    tok_r = lax.broadcasted_iota(jnp.int32, (qlen, lanes), 0)
    tok_l = lax.broadcasted_iota(jnp.int32, (qlen, lanes), 1)
    spread = jnp.where(tok_l // nq == tok_r, 1.0, 0.0).astype(BF16)
    qm = qmbuf[...].astype(F32).astype(BF16)
    qmw = jnp.dot(qm, spread, preferred_element_type=F32)
    qsub = lax.broadcasted_iota(jnp.int32, (nq, lanes), 0)
    qlan = lax.broadcasted_iota(jnp.int32, (nq, lanes), 1)
    qmu = jnp.sum(jnp.where(qlan % nq == qsub, qmw, 0.0), axis=0, keepdims=True)
    pr = lax.broadcasted_iota(jnp.int32, (lanes, lanes), 0)
    pc = lax.broadcasted_iota(jnp.int32, (lanes, lanes), 1)
    perm = jnp.where((pr % qlen) * nq + pr // qlen == pc, qmu, 0.0).astype(BF16)

    def project(block):
        out = jnp.dot(block, wbuf[...], preferred_element_type=F32)
        ss = jnp.sum(out * out, axis=-1, keepdims=True)
        return out * lax.rsqrt(jnp.maximum(ss, 1e-24))

    copies[0].wait()
    copies[1].wait()
    qn = project(qbuf[...]).T.astype(BF16)
    qt = jnp.dot(qn, perm, preferred_element_type=F32).astype(BF16)
    qt_all[me] = qt

    copies[3].wait()
    dm8[...] = jnp.zeros_like(dm8)
    dm8[0:ndoc, :] = dmbuf[...].astype(F32)
    mt = dm8[...].T
    for j in range(ndoc):
        mcol[pl.ds(j * dlen, dlen), :] = jnp.broadcast_to(mt[:, j:j + 1], (dlen, proj)).astype(BF16)

    pl.semaphore_wait(barrier, nchip * CORES - 1)

    def q_send(k):
        cy, cx, cid = rel(k)
        return pltpu.make_async_remote_copy(
            src_ref=qt_all.at[me], dst_ref=qt_all.at[me],
            send_sem=qsend.at[k], recv_sem=qrecv.at[chip],
            device_id=dev(cy, cx, core), device_id_type=MESH)

    def q_recv(k):
        cy, cx, cid = rel(k)
        slot = cid * CORES + core
        return pltpu.make_async_remote_copy(
            src_ref=qt_all.at[slot], dst_ref=qt_all.at[slot],
            send_sem=qsend.at[k], recv_sem=qrecv.at[cid],
            device_id=dev(cy, cx, core), device_id_type=MESH)

    def forward(k):
        _, _, cid = rel(k)
        slot = cid * CORES + core
        return pltpu.make_async_remote_copy(
            src_ref=qt_all.at[slot], dst_ref=qt_all.at[slot],
            send_sem=fsend.at[k], recv_sem=frecv.at[cid],
            device_id=dev(y, x, other), device_id_type=MESH)

    def forwarded(k):
        _, _, cid = rel(k)
        slot = cid * CORES + other
        return pltpu.make_async_remote_copy(
            src_ref=qt_all.at[slot], dst_ref=qt_all.at[slot],
            send_sem=fsend.at[k], recv_sem=frecv.at[cid],
            device_id=dev(y, x, other), device_id_type=MESH)

    forward(0).start()
    for k in range(1, nchip):
        q_send(k).start()

    for j in range(ndoc):
        for c in range(per_doc):
            cc = j * per_doc + c
            doc_copy(cc).wait()
            part = pl.ds(cc * chunk, chunk)
            p_buf[part, :] = project(dbuf[part, :]).astype(BF16)
        row = dm8[j:j + 1, :]
        pos = lax.broadcasted_iota(jnp.int32, (1, dlen), 1).astype(F32)
        first = jnp.min(jnp.where(row > 0, pos, float(dlen)), axis=-1, keepdims=True)
        pick = jnp.where(pos == first, 1.0, 0.0).astype(BF16)
        part = pl.ds(j * dlen, dlen)
        pj = p_buf[part, :]
        fill = jnp.dot(pick, pj, preferred_element_type=F32).astype(BF16)
        m = mcol[part, :]
        p_buf[part, :] = pj * m + fill * (1 - m)

    def arrive(k):
        if k > 0:
            q_recv(k).wait_recv()
            forward(k).start()

    for k in range(group):
        arrive(k)
    s_acc = jnp.zeros((8, lanes), F32)
    for g in range(0, nchip, group):
        for k in range(g + group, min(g + 2 * group, nchip)):
            arrive(k)
        ids = []
        for k in range(g, g + group):
            forwarded(k).wait_recv()
            _, _, cid = rel(k)
            ids += [cid * CORES, cid * CORES + 1]
        rhs = jnp.concatenate([qt_all[i] for i in ids], axis=1)
        width = rhs.shape[1]
        best = jnp.zeros((8, width), F32)
        wsub = lax.broadcasted_iota(jnp.int32, (8, width), 0)
        for j in range(ndoc):
            acc = None
            for c in range(dlen // rows):
                lhs = p_buf[pl.ds(j * dlen + c * rows, rows), :]
                s = jnp.dot(lhs, rhs, preferred_element_type=F32)
                s = jnp.max(s.reshape(rows // 8, 8, width), axis=0)
                acc = s if acc is None else jnp.maximum(acc, s)
            best = jnp.where(wsub == j, jnp.max(acc, axis=0, keepdims=True), best)
        for n, i in enumerate(ids):
            v = best[:, n * lanes:(n + 1) * lanes]
            shift = lanes // 2
            while shift >= nq:
                v = v + pltpu.roll(v, shift, 1)
                shift //= 2
            s_acc = jnp.where(lane // nq == i, v, s_acc)

    s_all[me] = s_acc[:ndoc, :]

    def s_send(k, c):
        cy, cx, cid = rel(k)
        return pltpu.make_async_remote_copy(
            src_ref=s_all.at[me], dst_ref=s_all.at[me],
            send_sem=ssend.at[k * CORES + c], recv_sem=srecv.at[me],
            device_id=dev(cy, cx, c if k > 0 else other), device_id_type=MESH)

    def s_recv(k, c):
        cy, cx, cid = rel(k)
        c = c if k > 0 else other
        slot = cid * CORES + c
        return pltpu.make_async_remote_copy(
            src_ref=s_all.at[slot], dst_ref=s_all.at[slot],
            send_sem=ssend.at[0], recv_sem=srecv.at[slot],
            device_id=dev(cy, cx, c), device_id_type=MESH)

    peers = [(k, c) for k in range(nchip - 1, 0, -1) for c in range(CORES)] + [(0, 1)]
    for k, c in peers:
        s_send(k, c).start()
    copies[4].wait()
    temp = tbuf[0, 0]
    for k in range(1, nchip):
        q_send(k).wait_send()
    for k in range(nchip):
        forward(k).wait_send()
    for k, c in peers[::-1]:
        s_recv(k, c).wait_recv()

    logits = s_all[...] / temp
    top = jnp.max(jnp.max(logits, axis=0), axis=0, keepdims=True)
    total = jnp.sum(jnp.sum(jnp.exp(logits - top[None]), axis=0), axis=0, keepdims=True)
    dd = lax.broadcasted_iota(jnp.int32, logits.shape, 0)
    dj = lax.broadcasted_iota(jnp.int32, logits.shape, 1)
    dl = lax.broadcasted_iota(jnp.int32, logits.shape, 2)
    own = jnp.where(dd * nq + dj == dl, logits, 0.0)
    diag = jnp.sum(jnp.sum(own, axis=0), axis=0, keepdims=True)
    losses = top + jnp.log(total) - diag
    mean_ref[0] = jnp.sum(losses) / (ndev * nq)
    l1 = lax.broadcasted_iota(jnp.int32, losses.shape, 1)
    for q in range(nq):
        loss_ref[q] = jnp.sum(jnp.where(l1 == me * nq + q, losses, 0.0))

    for k, c in peers:
        s_send(k, c).wait_send()


def solution(mesh):
    ny = mesh.shape["data2"]
    nx = mesh.shape["data"] // CORES
    row_spec = P(("replica", "data2", "data"))
    tok_spec = P(("replica", "data2", "data"), None, None)
    mask_spec = P(("replica", "data2", "data"), None)

    def local_step(query_hidden, doc_hidden, w_proj, query_mask, doc_mask, temperature):
        nq, qlen, hidden = query_hidden.shape
        ndoc, dlen, _ = doc_hidden.shape
        proj = w_proj.shape[1]
        nchip = ny * nx
        ndev = nchip * CORES
        chunk, rows = 256, 128
        cfg = (ny, nx, nq, qlen, ndoc, dlen, chunk, rows)
        nchunk = ndoc * dlen // chunk
        dma = pltpu.SemaphoreType.DMA
        return pl.pallas_call(
            functools.partial(kernel, cfg),
            out_shape=(jax.ShapeDtypeStruct((nq,), F32), jax.ShapeDtypeStruct((1,), F32)),
            in_specs=[pl.BlockSpec(memory_space=pl.ANY)] * 6,
            out_specs=(pl.BlockSpec(memory_space=pltpu.SMEM), pl.BlockSpec(memory_space=pltpu.SMEM)),
            scratch_shapes=[
                pltpu.VMEM((nq * qlen, hidden), BF16),
                pltpu.VMEM((ndoc * dlen, hidden), BF16),
                pltpu.VMEM((hidden, proj), BF16),
                pltpu.VMEM((nq, qlen), jnp.int32),
                pltpu.VMEM((ndoc, dlen), jnp.int32),
                pltpu.VMEM((8, dlen), F32),
                pltpu.SMEM((1, 1), F32),
                pltpu.VMEM((ndev, proj, nq * qlen), BF16),
                pltpu.VMEM((ndoc * dlen, proj), BF16),
                pltpu.VMEM((ndoc * dlen, proj), BF16),
                pltpu.VMEM((ndev, ndoc, ndev * nq), F32),
                dma((5,)), dma((nchunk,)),
                dma((nchip,)), dma((nchip,)), dma((nchip,)), dma((nchip,)),
                dma((ndev,)), dma((ndev,)),
            ],
            compiler_params=pltpu.CompilerParams(
                collective_id=0, has_side_effects=True, vmem_limit_bytes=60 * 1024 * 1024),
        )(query_hidden.reshape(nq * qlen, hidden), doc_hidden.reshape(ndoc * dlen, hidden),
          w_proj, query_mask, doc_mask, temperature.reshape(1, 1))

    return jax.shard_map(local_step, mesh=mesh, in_specs=(tok_spec, tok_spec, P(None, None), mask_spec, mask_spec, P()), out_specs=(row_spec, P("replica")), check_vma=False)
```

```python
import functools

import jax
import jax.numpy as jnp
from jax import lax
from jax.experimental import pallas as pl
from jax.experimental.pallas import tpu as pltpu
from jax.sharding import PartitionSpec as P

MESH = pl.DeviceIdType.MESH
F32 = jnp.float32
BF16 = jnp.bfloat16
CORES = 2


def offsets(n):
    return sorted(range(1, n), key=lambda o: (min(o, n - o), o))


def kernel(cfg, q_hbm, d_hbm, w_hbm, qm_hbm, dm_hbm, temp_hbm, out_ref,
           qbuf, dbuf, wbuf, qmbuf, dmbuf, dm8, tbuf, qt_all, p_buf, mcol, s_all,
           insem, dsem, qrecv, frecv, sems):
    ny, nx, nq, qlen, ndoc, dlen, rows, depth = cfg
    nchip = ny * nx
    ndev = nchip * CORES
    pass_at = 2
    proj = w_hbm.shape[1]
    lanes = nq * qlen
    na, nb = ny, nx
    y = lax.axis_index("data2")
    xc = lax.axis_index("data")
    x = xc // CORES
    core = xc % CORES
    other = 1 - core
    me = (y * nx + x) * CORES + core
    turn = core if ny == nx else 0
    turn_o = other if ny == nx else 0
    a, b = y + turn * (x - y), x + turn * (y - x)
    ao, bo = y + turn_o * (x - y), x + turn_o * (y - x)
    near = [o for o in offsets(na) if min(o, na - o) == 1]
    far = [o for o in offsets(na) if min(o, na - o) > 1]

    def dev(cy, cx, c):
        return {"data2": cy, "data": cx * CORES + c}

    def plane_dev(pa, pb):
        return dev(pa + turn * (pb - pa), pb + turn * (pa - pb), core)

    def step(p, o, n):
        return lax.rem(p + o, n)

    def row_of(c, pa):
        return pl.ds((c * na + pa) * nb, nb)

    def owners(c, t, pa):
        return [((pa + t * (i - pa)) * nx + i + t * (pa - i)) * CORES + c for i in range(nb)]

    def wait_bytes(buf, n, sem):
        pltpu.make_async_copy(buf.at[pl.ds(0, n)], buf.at[pl.ds(0, n)], sem).wait()

    copies = [
        pltpu.make_async_copy(q_hbm, qbuf, insem.at[0]),
        pltpu.make_async_copy(w_hbm, wbuf, insem.at[1]),
        pltpu.make_async_copy(qm_hbm, qmbuf, insem.at[2]),
        pltpu.make_async_copy(dm_hbm, dmbuf, insem.at[3]),
        pltpu.make_async_copy(temp_hbm, tbuf, insem.at[4]),
    ]
    for cp in copies:
        cp.start()

    def doc_copy(j):
        part = pl.ds(j * dlen, dlen)
        return pltpu.make_async_copy(d_hbm.at[part], dbuf.at[part], dsem.at[j])

    for j in range(depth):
        doc_copy(j).start()

    barrier = pltpu.get_barrier_semaphore()
    ring1 = [plane_dev(a, step(b, o, nb)) for o in offsets(nb)[::-1]]
    ring2 = [plane_dev(step(a, o, na), b) for o in offsets(na)]
    partner = dev(y, x, other)
    for d in ring2[::-1] + ring1 + [partner]:
        pl.semaphore_signal(barrier, inc=1, device_id=d, device_id_type=MESH)

    copies[2].wait()
    tok_r = lax.broadcasted_iota(jnp.int32, (qlen, lanes), 0)
    tok_l = lax.broadcasted_iota(jnp.int32, (qlen, lanes), 1)
    spread = jnp.where(tok_l // nq == tok_r, 1.0, 0.0).astype(BF16)
    qm = qmbuf[...].astype(F32).astype(BF16)
    qmw = jnp.dot(qm, spread, preferred_element_type=F32)
    qsub = lax.broadcasted_iota(jnp.int32, (nq, lanes), 0)
    qlan = lax.broadcasted_iota(jnp.int32, (nq, lanes), 1)
    qmu = jnp.sum(jnp.where(qlan % nq == qsub, qmw, 0.0), axis=0, keepdims=True)
    pr = lax.broadcasted_iota(jnp.int32, (lanes, lanes), 0)
    pc = lax.broadcasted_iota(jnp.int32, (lanes, lanes), 1)
    perm = jnp.where((pr % qlen) * nq + pr // qlen == pc, qmu, 0.0).astype(BF16)

    def project(block):
        out = jnp.dot(block, wbuf[...], preferred_element_type=F32)
        ss = jnp.sum(out * out, axis=-1, keepdims=True)
        return out * lax.rsqrt(jnp.maximum(ss, 1e-24))

    copies[0].wait()
    copies[1].wait()
    qn = project(qbuf[...]).T.astype(BF16)
    mine = (core * na + a) * nb + b
    qt_all[mine] = jnp.dot(qn, perm, preferred_element_type=F32).astype(BF16)

    copies[3].wait()
    dm8[...] = jnp.zeros_like(dm8)
    dm8[0:ndoc, :] = dmbuf[...].astype(F32)

    pl.semaphore_wait(barrier, na + nb - 1)

    def send(part, d, send_sem, recv_sem):
        pltpu.make_async_remote_copy(
            src_ref=qt_all.at[part], dst_ref=qt_all.at[part], send_sem=send_sem, recv_sem=recv_sem,
            device_id=d, device_id_type=MESH).start()

    def pass_rows():
        wait_bytes(qt_all, nb - 1, qrecv.at[0])
        for o, d in zip(offsets(na), ring2):
            send(row_of(core, a), d, sems.at[0], qrecv.at[1 if o in near else 2])
        send(row_of(core, a), partner, sems.at[1], frecv.at[0])

    def hand_over(which, steps):
        wait_bytes(qt_all, len(steps) * nb, qrecv.at[which])
        for o in steps:
            send(row_of(core, step(a, o, na)), partner, sems.at[1], frecv.at[which])

    for d in ring1:
        send(pl.ds(mine, 1), d, sems.at[0], qrecv.at[0])

    mt = dm8[...].T

    def fill(j):
        part = pl.ds(j * dlen, dlen)
        row = dm8[j:j + 1, :]
        pos = lax.broadcasted_iota(jnp.int32, (1, dlen), 1).astype(F32)
        first = jnp.min(jnp.where(row > 0, pos, float(dlen)), axis=-1, keepdims=True)
        pick = jnp.where(pos == first, 1.0, 0.0).astype(BF16)
        pj = p_buf[part, :]
        token = jnp.dot(pick, pj, preferred_element_type=F32).astype(BF16)
        m = mcol[part, :]
        p_buf[part, :] = pj * m + token * (1 - m)

    for j in range(ndoc):
        doc_copy(j).wait()
        if j + depth < ndoc:
            doc_copy(j + depth).start()
        if j == pass_at:
            pass_rows()
        for c in range(dlen // rows):
            part = pl.ds(j * dlen + c * rows, rows)
            p_buf[part, :] = project(dbuf[part, :]).astype(BF16)
        mcol[pl.ds(j * dlen, dlen), :] = jnp.broadcast_to(mt[:, j:j + 1], (dlen, proj)).astype(BF16)
        if j > 0:
            fill(j - 1)

    lane = lax.broadcasted_iota(jnp.int32, (8, lanes), 1)
    width = nb * lanes
    wsub = lax.broadcasted_iota(jnp.int32, (8, width), 0)

    def tail(s_acc, best, ids):
        for n, i in enumerate(ids):
            v = best[:, n * lanes:(n + 1) * lanes]
            shift = lanes // 2
            while shift >= nq:
                v = v + pltpu.roll(v, shift, 1)
                shift //= 2
            s_acc = jnp.where(lane // nq == i, v, s_acc)
        return s_acc

    def own(o):
        return core, turn, step(a, o, na)

    def others(o):
        return other, turn_o, step(ao, o, na)

    plan = [(own(0), None), (others(0), lambda: wait_bytes(qt_all, nb, frecv.at[0]))]
    for which, steps in ((1, near), (2, far)):
        todo = [(own(o), None) for o in steps] + [(others(o), None) for o in steps]
        todo[0] = (todo[0][0], functools.partial(hand_over, which, steps))
        todo[len(steps)] = (todo[len(steps)][0], functools.partial(wait_bytes, qt_all, len(steps) * nb, frecv.at[which]))
        plan += todo

    s_acc = jnp.zeros((8, lanes), F32)
    pending = []
    for g, ((c, t, pa), ready) in enumerate(plan):
        if ready is not None:
            ready()
        if g == 0:
            fill(ndoc - 1)
        rhs = qt_all[row_of(c, pa)]
        rhs = jnp.concatenate([rhs[i] for i in range(nb)], axis=1)
        best = jnp.zeros((8, width), F32)
        for j in range(ndoc):
            s = jnp.dot(p_buf[pl.ds(j * dlen, dlen), :], rhs, preferred_element_type=F32)
            s = jnp.max(s.reshape(dlen // 8, 8, width), axis=0)
            best = jnp.where(wsub == j, jnp.max(s, axis=0, keepdims=True), best)
        for item in pending:
            s_acc = tail(s_acc, *item)
        pending = [(best, owners(c, t, pa))]
    for item in pending:
        s_acc = tail(s_acc, *item)
    copies[4].wait()
    s_all[me] = s_acc[:ndoc, :] / tbuf[0]

    peers = [(oy, ox, c) for oy in range(ny) for ox in range(nx) for c in range(CORES)][1:]
    peers.sort(key=lambda p: -min(p[0], ny - p[0]) - min(p[1], nx - p[1]))
    for oy, ox, c in peers:
        pltpu.make_async_remote_copy(
            src_ref=s_all.at[me], dst_ref=s_all.at[me],
            send_sem=sems.at[2], recv_sem=sems.at[3],
            device_id=dev(step(y, oy, ny), step(x, ox, nx), step(core, c, CORES)), device_id_type=MESH).start()
    wait_bytes(qt_all, nb - 1 + (na - 1) * nb, sems.at[0])
    wait_bytes(qt_all, nchip, sems.at[1])
    wait_bytes(s_all, ndev - 1, sems.at[3])

    logits = s_all[...]
    top = jnp.max(jnp.max(logits, axis=0), axis=0, keepdims=True)
    total = jnp.sum(jnp.sum(jnp.exp(logits - top[None]), axis=0), axis=0, keepdims=True)
    dd = lax.broadcasted_iota(jnp.int32, logits.shape, 0)
    dj = lax.broadcasted_iota(jnp.int32, logits.shape, 1)
    dl = lax.broadcasted_iota(jnp.int32, logits.shape, 2)
    diag = jnp.sum(jnp.sum(jnp.where(dd * nq + dj == dl, logits, 0.0), axis=0), axis=0, keepdims=True)
    losses = top + jnp.log(total) - diag
    nrow = ndev * nq
    home = pltpu.roll(jnp.broadcast_to(losses, (8, nrow)), lax.rem(nrow - me * nq, nrow), 1)
    mean = jnp.sum(losses, axis=1, keepdims=True) / nrow
    out_ref[...] = jnp.where(lax.broadcasted_iota(jnp.int32, home.shape, 0) == 0, home, mean)

    wait_bytes(s_all, ndev - 1, sems.at[2])


def finish(vec_ref, loss_ref, mean_ref):
    loss_ref[...] = vec_ref[0, :loss_ref.shape[0]]
    mean_ref[...] = vec_ref[1, :1]


def solution(mesh):
    ny = mesh.shape["data2"]
    nx = mesh.shape["data"] // CORES
    row_spec = P(("replica", "data2", "data"))
    tok_spec = P(("replica", "data2", "data"), None, None)
    mask_spec = P(("replica", "data2", "data"), None)

    def local_step(query_hidden, doc_hidden, w_proj, query_mask, doc_mask, temperature):
        nq, qlen, hidden = query_hidden.shape
        ndoc, dlen, _ = doc_hidden.shape
        proj = w_proj.shape[1]
        ndev = ny * nx * CORES
        rows, depth = 128, 2
        cfg = (ny, nx, nq, qlen, ndoc, dlen, rows, depth)
        dma = pltpu.SemaphoreType.DMA
        vec = pl.pallas_call(
            functools.partial(kernel, cfg),
            out_shape=jax.ShapeDtypeStruct((8, ndev * nq), F32),
            in_specs=[pl.BlockSpec(memory_space=pl.ANY)] * 6,
            out_specs=pl.BlockSpec(memory_space=pltpu.VMEM),
            scratch_shapes=[
                pltpu.VMEM((nq * qlen, hidden), BF16),
                pltpu.VMEM((ndoc * dlen, hidden), BF16),
                pltpu.VMEM((hidden, proj), BF16),
                pltpu.VMEM((nq, qlen), jnp.int32),
                pltpu.VMEM((ndoc, dlen), jnp.int32),
                pltpu.VMEM((8, dlen), F32),
                pltpu.SMEM((1,), F32),
                pltpu.VMEM((ndev, proj, nq * qlen), BF16),
                pltpu.VMEM((ndoc * dlen, proj), BF16),
                pltpu.VMEM((ndoc * dlen, proj), BF16),
                pltpu.VMEM((ndev, ndoc, ndev * nq), F32),
                dma((5,)), dma((ndoc,)), dma((3,)), dma((3,)), dma((4,)),
            ],
            compiler_params=pltpu.CompilerParams(
                collective_id=0, has_side_effects=True, vmem_limit_bytes=60 * 1024 * 1024),
        )(query_hidden.reshape(nq * qlen, hidden), doc_hidden.reshape(ndoc * dlen, hidden),
          w_proj, query_mask, doc_mask, temperature.reshape(1))
        return pl.pallas_call(
            finish,
            out_shape=(jax.ShapeDtypeStruct((nq,), F32), jax.ShapeDtypeStruct((1,), F32)),
            in_specs=[pl.BlockSpec(memory_space=pltpu.VMEM)],
            out_specs=(pl.BlockSpec(memory_space=pltpu.VMEM), pl.BlockSpec(memory_space=pltpu.VMEM)),
        )(vec)

    return jax.shard_map(local_step, mesh=mesh, in_specs=(tok_spec, tok_spec, P(None, None), mask_spec, mask_spec, P()), out_specs=(row_spec, P("replica")), check_vma=False)
```

```python
import functools

import jax
import jax.numpy as jnp
from jax import lax
from jax.experimental import pallas as pl
from jax.experimental.pallas import tpu as pltpu
from jax.sharding import PartitionSpec as P

MESH = pl.DeviceIdType.MESH
F32 = jnp.float32
BF16 = jnp.bfloat16
CORES = 2


def offsets(n):
    return sorted(range(1, n), key=lambda o: (min(o, n - o), o))


def kernel(cfg, q_hbm, d_hbm, w_hbm, qm_hbm, dm_hbm, temp_hbm, out_ref,
           qbuf, dbuf, wbuf, qmbuf, dmbuf, dm8, tbuf, qt_all, p_buf, mcol, s_all,
           insem, dsem, qrecv, frecv, sems):
    ny, nx, nq, qlen, ndoc, dlen, rows, depth = cfg
    nchip = ny * nx
    ndev = nchip * CORES
    pass_at = 3
    wide = 4
    proj = w_hbm.shape[1]
    lanes = nq * qlen
    na, nb = ny, nx
    y = lax.axis_index("data2")
    xc = lax.axis_index("data")
    x = xc // CORES
    core = xc % CORES
    other = 1 - core
    me = (y * nx + x) * CORES + core
    turn = core if ny == nx else 0
    turn_o = other if ny == nx else 0
    a, b = y + turn * (x - y), x + turn * (y - x)
    ao, bo = y + turn_o * (x - y), x + turn_o * (y - x)
    near = [o for o in offsets(na) if min(o, na - o) == 1]
    far = [o for o in offsets(na) if min(o, na - o) > 1]

    def dev(cy, cx, c):
        return {"data2": cy, "data": cx * CORES + c}

    def plane_dev(pa, pb):
        return dev(pa + turn * (pb - pa), pb + turn * (pa - pb), core)

    def step(p, o, n):
        return lax.rem(p + o, n)

    def block(c, i, j):
        c, t, pa, pb = (core, turn, a, b) if c == 0 else (other, turn_o, ao, bo)
        pa, pb = step(pa, i, na), step(pb, j, nb)
        return (c * na + pa) * nb + pb, ((pa + t * (pb - pa)) * nx + pb + t * (pa - pb)) * CORES + c

    def wait_bytes(buf, n, sem):
        pltpu.make_async_copy(buf.at[pl.ds(0, n)], buf.at[pl.ds(0, n)], sem).wait()

    barrier = pltpu.get_barrier_semaphore()
    ring1 = {o: plane_dev(a, step(b, o, nb)) for o in offsets(nb)[::-1]}
    ring2 = {o: plane_dev(step(a, o, na), b) for o in offsets(na)[::-1]}
    partner = dev(y, x, other)
    for d in [*ring2.values(), *ring1.values(), partner]:
        pl.semaphore_signal(barrier, inc=1, device_id=d, device_id_type=MESH)

    copies = [
        pltpu.make_async_copy(q_hbm, qbuf, insem.at[0]),
        pltpu.make_async_copy(w_hbm, wbuf, insem.at[1]),
        pltpu.make_async_copy(qm_hbm, qmbuf, insem.at[2]),
        pltpu.make_async_copy(dm_hbm, dmbuf, insem.at[3]),
        pltpu.make_async_copy(temp_hbm, tbuf, insem.at[4]),
    ]
    for cp in copies:
        cp.start()

    def doc_copy(j):
        part = pl.ds(j * dlen, dlen)
        return pltpu.make_async_copy(d_hbm.at[part], dbuf.at[part], dsem.at[j])

    for j in range(depth):
        doc_copy(j).start()

    copies[2].wait()
    tok_r = lax.broadcasted_iota(jnp.int32, (qlen, lanes), 0)
    tok_l = lax.broadcasted_iota(jnp.int32, (qlen, lanes), 1)
    spread = jnp.where(tok_l // nq == tok_r, 1.0, 0.0).astype(BF16)
    qm = qmbuf[...].astype(F32).astype(BF16)
    qmw = jnp.dot(qm, spread, preferred_element_type=F32)
    qsub = lax.broadcasted_iota(jnp.int32, (nq, lanes), 0)
    qlan = lax.broadcasted_iota(jnp.int32, (nq, lanes), 1)
    qmu = jnp.sum(jnp.where(qlan % nq == qsub, qmw, 0.0), axis=0, keepdims=True)
    pr = lax.broadcasted_iota(jnp.int32, (lanes, lanes), 0)
    pc = lax.broadcasted_iota(jnp.int32, (lanes, lanes), 1)
    perm = jnp.where((pr % qlen) * nq + pr // qlen == pc, qmu, 0.0).astype(BF16)

    def project(block):
        out = jnp.dot(block, wbuf[...], preferred_element_type=F32)
        ss = jnp.sum(out * out, axis=-1, keepdims=True)
        return out * lax.rsqrt(jnp.maximum(ss, 1e-24))

    copies[0].wait()
    copies[1].wait()
    for j in range(depth, min(depth + 1, ndoc)):
        doc_copy(j).start()
    qn = project(qbuf[...]).T.astype(BF16)
    mine = block(0, 0, 0)[0]
    qt_all[mine] = jnp.dot(qn, perm, preferred_element_type=F32).astype(BF16)

    copies[3].wait()
    dm8[...] = jnp.zeros_like(dm8)
    dm8[0:ndoc, :] = dmbuf[...].astype(F32)

    pl.semaphore_wait(barrier, na + nb - 1)

    def send(slot, d, send_sem, recv_sem):
        pltpu.make_async_remote_copy(
            src_ref=qt_all.at[slot], dst_ref=qt_all.at[slot], send_sem=send_sem, recv_sem=recv_sem,
            device_id=d, device_id_type=MESH).start()

    cross1 = [(0, o) for o in offsets(nb)]
    cross2 = [(o, 0) for o in offsets(na)]
    rest = [(i, j) for i in near for j in offsets(nb)] + [(i, j) for i in far for j in offsets(nb)]

    def pass_cross():
        wait_bytes(qt_all, len(cross1) + len(cross2), qrecv.at[0])
        wait_bytes(qt_all, 1, frecv.at[0])
        for i, j in cross1:
            for o in near:
                send(block(0, i, j)[0], ring2[o], sems.at[0], qrecv.at[1])
        for i in far:
            for o in offsets(nb):
                send(block(0, i, 0)[0], ring1[o], sems.at[0], qrecv.at[1])
        for i, j in cross1 + cross2:
            send(block(0, i, j)[0], partner, sems.at[1], frecv.at[1])

    def pass_rest():
        wait_bytes(qt_all, len(rest), qrecv.at[1])
        for i, j in rest:
            send(block(0, i, j)[0], partner, sems.at[1], frecv.at[2])

    for d in [*ring2.values(), *ring1.values()]:
        send(mine, d, sems.at[0], qrecv.at[0])
    send(mine, partner, sems.at[1], frecv.at[0])

    for j in range(depth + 1, ndoc):
        doc_copy(j).start()
    mt = dm8[...].T

    def fill(j):
        part = pl.ds(j * dlen, dlen)
        row = dm8[j:j + 1, :]
        pos = lax.broadcasted_iota(jnp.int32, (1, dlen), 1).astype(F32)
        first = jnp.min(jnp.where(row > 0, pos, float(dlen)), axis=-1, keepdims=True)
        pick = jnp.where(pos == first, 1.0, 0.0).astype(BF16)
        pj = p_buf[part, :]
        token = jnp.dot(pick, pj, preferred_element_type=F32).astype(BF16)
        m = mcol[part, :]
        p_buf[part, :] = pj * m + token * (1 - m)

    for j in range(ndoc):
        doc_copy(j).wait()
        if j == pass_at:
            pass_cross()
        for c in range(dlen // rows):
            part = pl.ds(j * dlen + c * rows, rows)
            p_buf[part, :] = project(dbuf[part, :]).astype(BF16)
        mcol[pl.ds(j * dlen, dlen), :] = jnp.broadcast_to(mt[:, j:j + 1], (dlen, proj)).astype(BF16)
        if j > 0:
            fill(j - 1)

    lane = lax.broadcasted_iota(jnp.int32, (8, lanes), 1)
    width = wide * lanes
    wsub = lax.broadcasted_iota(jnp.int32, (8, width), 0)

    def tail(s_acc, best, ids):
        for n, i in enumerate(ids):
            v = best[:, n * lanes:(n + 1) * lanes]
            shift = lanes // 2
            while shift >= nq:
                v = v + pltpu.roll(v, shift, 1)
                shift //= 2
            s_acc = jnp.where(lane // nq == i, v, s_acc)
        return s_acc

    arrivals = [
        ([(0, 0, 0)] + [(0, *o) for o in cross1] + [(1, 0, 0)] + [(0, *o) for o in cross2], None),
        ([(1, *o) for o in cross1 + cross2], lambda: wait_bytes(qt_all, len(cross1) + len(cross2), frecv.at[1])),
        ([(0, *o) for o in rest], pass_rest),
        ([(1, *o) for o in rest], lambda: wait_bytes(qt_all, len(rest), frecv.at[2])),
    ]
    queue = [(where, ready if n == 0 else None) for blocks, ready in arrivals for n, where in enumerate(blocks)]

    s_acc = jnp.zeros((8, lanes), F32)
    pending = []
    for g in range(0, len(queue), wide):
        for _, ready in queue[g:g + wide]:
            if ready is not None:
                ready()
        if g == 0:
            fill(ndoc - 1)
        here = [block(*where) for where, _ in queue[g:g + wide]]
        rhs = jnp.concatenate([qt_all[slot] for slot, _ in here], axis=1)
        best = jnp.zeros((8, width), F32)
        for j in range(ndoc):
            s = jnp.dot(p_buf[pl.ds(j * dlen, dlen), :], rhs, preferred_element_type=F32)
            s = jnp.max(s.reshape(dlen // 8, 8, width), axis=0)
            best = jnp.where(wsub == j, jnp.max(s, axis=0, keepdims=True), best)
            if j == 0:
                for item in pending:
                    s_acc = tail(s_acc, *item)
        pending = [(best, [i for _, i in here])]
    for item in pending:
        s_acc = tail(s_acc, *item)
    copies[4].wait()
    s_all[me] = s_acc[:ndoc, :] / tbuf[0]

    peers = [(oy, ox, c) for oy in range(ny) for ox in range(nx) for c in range(CORES)][1:]
    peers.sort(key=lambda p: -min(p[0], ny - p[0]) - min(p[1], nx - p[1]))
    for oy, ox, c in peers:
        pltpu.make_async_remote_copy(
            src_ref=s_all.at[me], dst_ref=s_all.at[me],
            send_sem=sems.at[2], recv_sem=sems.at[3],
            device_id=dev(step(y, oy, ny), step(x, ox, nx), step(core, c, CORES)), device_id_type=MESH).start()
    wait_bytes(qt_all, nchip - 1, sems.at[0])
    wait_bytes(qt_all, nchip, sems.at[1])
    wait_bytes(s_all, ndev - 1, sems.at[3])

    logits = s_all[...]
    top = jnp.max(jnp.max(logits, axis=0), axis=0, keepdims=True)
    total = jnp.sum(jnp.sum(jnp.exp(logits - top[None]), axis=0), axis=0, keepdims=True)
    dd = lax.broadcasted_iota(jnp.int32, logits.shape, 0)
    dj = lax.broadcasted_iota(jnp.int32, logits.shape, 1)
    dl = lax.broadcasted_iota(jnp.int32, logits.shape, 2)
    diag = jnp.sum(jnp.sum(jnp.where(dd * nq + dj == dl, logits, 0.0), axis=0), axis=0, keepdims=True)
    losses = top + jnp.log(total) - diag
    nrow = ndev * nq
    home = pltpu.roll(jnp.broadcast_to(losses, (8, nrow)), lax.rem(nrow - me * nq, nrow), 1)
    mean = jnp.sum(losses, axis=1, keepdims=True) / nrow
    out_ref[...] = jnp.where(lax.broadcasted_iota(jnp.int32, home.shape, 0) == 0, home, mean)

    wait_bytes(s_all, ndev - 1, sems.at[2])


def finish(vec_ref, loss_ref, mean_ref):
    loss_ref[...] = vec_ref[0, :loss_ref.shape[0]]
    mean_ref[...] = vec_ref[1, :1]


def solution(mesh):
    ny = mesh.shape["data2"]
    nx = mesh.shape["data"] // CORES
    row_spec = P(("replica", "data2", "data"))
    tok_spec = P(("replica", "data2", "data"), None, None)
    mask_spec = P(("replica", "data2", "data"), None)

    def local_step(query_hidden, doc_hidden, w_proj, query_mask, doc_mask, temperature):
        nq, qlen, hidden = query_hidden.shape
        ndoc, dlen, _ = doc_hidden.shape
        proj = w_proj.shape[1]
        ndev = ny * nx * CORES
        rows, depth = 128, 1
        cfg = (ny, nx, nq, qlen, ndoc, dlen, rows, depth)
        dma = pltpu.SemaphoreType.DMA
        vec = pl.pallas_call(
            functools.partial(kernel, cfg),
            out_shape=pltpu.VMEM((8, ndev * nq), F32),
            in_specs=[pl.BlockSpec(memory_space=pl.ANY)] * 6,
            out_specs=pl.BlockSpec(memory_space=pltpu.VMEM),
            scratch_shapes=[
                pltpu.VMEM((nq * qlen, hidden), BF16),
                pltpu.VMEM((ndoc * dlen, hidden), BF16),
                pltpu.VMEM((hidden, proj), BF16),
                pltpu.VMEM((nq, qlen), jnp.int32),
                pltpu.VMEM((ndoc, dlen), jnp.int32),
                pltpu.VMEM((8, dlen), F32),
                pltpu.SMEM((1,), F32),
                pltpu.VMEM((ndev, proj, nq * qlen), BF16),
                pltpu.VMEM((ndoc * dlen, proj), BF16),
                pltpu.VMEM((ndoc * dlen, proj), BF16),
                pltpu.VMEM((ndev, ndoc, ndev * nq), F32),
                dma((5,)), dma((ndoc,)), dma((2,)), dma((3,)), dma((4,)),
            ],
            compiler_params=pltpu.CompilerParams(
                collective_id=0, has_side_effects=True, vmem_limit_bytes=60 * 1024 * 1024),
        )(query_hidden.reshape(nq * qlen, hidden), doc_hidden.reshape(ndoc * dlen, hidden),
          w_proj, query_mask, doc_mask, temperature.reshape(1))
        return pl.pallas_call(
            finish,
            out_shape=(jax.ShapeDtypeStruct((nq,), F32), jax.ShapeDtypeStruct((1,), F32)),
            in_specs=[pl.BlockSpec(memory_space=pltpu.VMEM)],
            out_specs=(pl.BlockSpec(memory_space=pltpu.VMEM), pl.BlockSpec(memory_space=pltpu.VMEM)),
            compiler_params=pltpu.CompilerParams(vmem_limit_bytes=1024 * 1024),
        )(vec)

    return jax.shard_map(local_step, mesh=mesh, in_specs=(tok_spec, tok_spec, P(None, None), mask_spec, mask_spec, P()), out_specs=(row_spec, P("replica")), check_vma=False)
```

```python
import functools

import jax
import jax.numpy as jnp
from jax import lax
from jax.experimental import pallas as pl
from jax.experimental.pallas import tpu as pltpu
from jax.sharding import PartitionSpec as P

MESH = pl.DeviceIdType.MESH
F32 = jnp.float32
BF16 = jnp.bfloat16
WIDE = 4
FAR = 1e30
CORES = 2


def offsets(n):
    return sorted(range(1, n), key=lambda o: (min(o, n - o), o))


def kernel(cfg, q_hbm, d_hbm, w_hbm, qm_hbm, dm_hbm, temp_hbm, out_ref,
           qbuf, dbuf, wbuf, qmbuf, dmbuf, dm8, tbuf, qt_all, p_buf, skip, pick, s_all,
           insem, dsem, qrecv, frecv, sems):
    ny, nx, nq, qlen, ndoc, dlen, rows, depth = cfg
    nchip = ny * nx
    ndev = nchip * CORES
    pass_at = 3
    wide = WIDE
    proj = w_hbm.shape[1]
    lanes = nq * qlen
    na, nb = ny, nx
    y = lax.axis_index("data2")
    xc = lax.axis_index("data")
    x = xc // CORES
    core = xc % CORES
    other = 1 - core
    me = (y * nx + x) * CORES + core
    turn = core if ny == nx else 0
    turn_o = other if ny == nx else 0
    a, b = y + turn * (x - y), x + turn * (y - x)
    ao, bo = y + turn_o * (x - y), x + turn_o * (y - x)
    near = [o for o in offsets(na) if min(o, na - o) == 1]
    far = [o for o in offsets(na) if min(o, na - o) > 1]

    def dev(cy, cx, c):
        return {"data2": cy, "data": cx * CORES + c}

    def plane_dev(pa, pb):
        return dev(pa + turn * (pb - pa), pb + turn * (pa - pb), core)

    def step(p, o, n):
        return lax.rem(p + o, n)

    def block(c, i, j):
        c, t, pa, pb = (core, turn, a, b) if c == 0 else (other, turn_o, ao, bo)
        pa, pb = step(pa, i, na), step(pb, j, nb)
        return (c * na + pa) * nb + pb, ((pa + t * (pb - pa)) * nx + pb + t * (pa - pb)) * CORES + c

    def wait_bytes(buf, n, sem):
        pltpu.make_async_copy(buf.at[pl.ds(0, n)], buf.at[pl.ds(0, n)], sem).wait()

    barrier = pltpu.get_barrier_semaphore()
    ring1 = {o: plane_dev(a, step(b, o, nb)) for o in offsets(nb)[::-1]}
    ring2 = {o: plane_dev(step(a, o, na), b) for o in offsets(na)[::-1]}
    partner = dev(y, x, other)
    for d in [*ring2.values(), *ring1.values(), partner]:
        pl.semaphore_signal(barrier, inc=1, device_id=d, device_id_type=MESH)

    copies = [
        pltpu.make_async_copy(q_hbm, qbuf, insem.at[0]),
        pltpu.make_async_copy(w_hbm, wbuf, insem.at[1]),
        pltpu.make_async_copy(qm_hbm, qmbuf, insem.at[2]),
        pltpu.make_async_copy(dm_hbm, dmbuf, insem.at[3]),
        pltpu.make_async_copy(temp_hbm, tbuf, insem.at[4]),
    ]
    for cp in copies:
        cp.start()

    def doc_copy(j):
        part = pl.ds(j * dlen, dlen)
        return pltpu.make_async_copy(d_hbm.at[part], dbuf.at[part], dsem.at[j])

    for j in range(depth):
        doc_copy(j).start()

    copies[2].wait()
    tok_r = lax.broadcasted_iota(jnp.int32, (qlen, lanes), 0)
    tok_l = lax.broadcasted_iota(jnp.int32, (qlen, lanes), 1)
    spread = jnp.where(tok_l // nq == tok_r, 1.0, 0.0).astype(BF16)
    qm = qmbuf[...].astype(F32).astype(BF16)
    qmw = jnp.dot(qm, spread, preferred_element_type=F32)
    qsub = lax.broadcasted_iota(jnp.int32, (nq, lanes), 0)
    qlan = lax.broadcasted_iota(jnp.int32, (nq, lanes), 1)
    qmu = jnp.sum(jnp.where(qlan % nq == qsub, qmw, 0.0), axis=0, keepdims=True)
    pr = lax.broadcasted_iota(jnp.int32, (lanes, lanes), 0)
    pc = lax.broadcasted_iota(jnp.int32, (lanes, lanes), 1)
    perm = jnp.where((pr % qlen) * nq + pr // qlen == pc, qmu, 0.0).astype(BF16)

    def project(block):
        out = jnp.dot(block, wbuf[...], preferred_element_type=F32)
        ss = jnp.sum(out * out, axis=-1, keepdims=True)
        return out * lax.rsqrt(jnp.maximum(ss, 1e-24))

    copies[0].wait()
    copies[1].wait()
    for j in range(depth, min(depth + 1, ndoc)):
        doc_copy(j).start()
    qn = project(qbuf[...]).T.astype(BF16)
    mine = block(0, 0, 0)[0]
    qt_all[mine] = jnp.dot(qn, perm, preferred_element_type=F32).astype(BF16)

    copies[3].wait()
    dm8[...] = jnp.ones_like(dm8)
    dm8[0:ndoc, :] = dmbuf[...].astype(F32)

    pl.semaphore_wait(barrier, na + nb - 1)

    def send(slot, d, send_sem, recv_sem):
        pltpu.make_async_remote_copy(
            src_ref=qt_all.at[slot], dst_ref=qt_all.at[slot], send_sem=send_sem, recv_sem=recv_sem,
            device_id=d, device_id_type=MESH).start()

    cross1 = [(0, o) for o in offsets(nb)]
    cross2 = [(o, 0) for o in offsets(na)]
    rest = [(i, j) for i in near for j in offsets(nb)] + [(i, j) for i in far for j in offsets(nb)]

    def pass_cross():
        wait_bytes(qt_all, len(cross1) + len(cross2), qrecv.at[0])
        wait_bytes(qt_all, 1, frecv.at[0])
        for i, j in cross1:
            for o in near:
                send(block(0, i, j)[0], ring2[o], sems.at[0], qrecv.at[1])
        for i in far:
            for o in offsets(nb):
                send(block(0, i, 0)[0], ring1[o], sems.at[0], qrecv.at[1])
        for i, j in cross1 + cross2:
            send(block(0, i, j)[0], partner, sems.at[1], frecv.at[1])

    def pass_rest():
        wait_bytes(qt_all, len(rest), qrecv.at[1])
        for i, j in rest:
            send(block(0, i, j)[0], partner, sems.at[1], frecv.at[2])

    for d in [*ring2.values(), *ring1.values()]:
        send(mine, d, sems.at[0], qrecv.at[0])
    send(mine, partner, sems.at[1], frecv.at[0])

    for j in range(depth + 1, ndoc):
        doc_copy(j).start()
    gone = jnp.concatenate([(dm8[...] - 1.0) * FAR, jnp.zeros((proj - 8, dlen), F32)], axis=0)
    skip[...] = gone.T.astype(BF16)
    erow = lax.broadcasted_iota(jnp.int32, pick.shape[1:], 0)
    for j in range(ndoc):
        pick[j] = jnp.where(erow == j, 1.0, 0.0).astype(BF16)

    for j in range(ndoc):
        doc_copy(j).wait()
        if j == pass_at:
            pass_cross()
        for c in range(dlen // rows):
            part = pl.ds(j * dlen + c * rows, rows)
            p_buf[part, :] = project(dbuf[part, :]).astype(BF16)

    lane = lax.broadcasted_iota(jnp.int32, (8, lanes), 1)
    width = wide * lanes
    wsub = lax.broadcasted_iota(jnp.int32, (8, width), 0)

    def tail(s_acc, best, ids):
        for n, i in enumerate(ids):
            v = best[:, n * lanes:(n + 1) * lanes]
            shift = lanes // 2
            while shift >= nq:
                v = v + pltpu.roll(v, shift, 1)
                shift //= 2
            s_acc = jnp.where(lane // nq == i, v, s_acc)
        return s_acc

    arrivals = [
        ([(0, 0, 0)] + [(0, *o) for o in cross1] + [(1, 0, 0)] + [(0, *o) for o in cross2], None),
        ([(1, *o) for o in cross1 + cross2], lambda: wait_bytes(qt_all, len(cross1) + len(cross2), frecv.at[1])),
        ([(0, *o) for o in rest], pass_rest),
        ([(1, *o) for o in rest], lambda: wait_bytes(qt_all, len(rest), frecv.at[2])),
    ]
    queue = [(where, ready if n == 0 else None) for blocks, ready in arrivals for n, where in enumerate(blocks)]

    s_acc = jnp.zeros((8, lanes), F32)
    pending = []
    for g in range(0, len(queue), wide):
        for _, ready in queue[g:g + wide]:
            if ready is not None:
                ready()
        here = [block(*where) for where, _ in queue[g:g + wide]]
        rhs = jnp.concatenate([qt_all[slot] for slot, _ in here], axis=1)
        best = jnp.zeros((8, width), F32)
        for j in range(ndoc):
            s = jnp.dot(jnp.concatenate([p_buf[pl.ds(j * dlen, dlen), :], skip[...]], axis=1),
                        jnp.concatenate([rhs, pick[j]], axis=0), preferred_element_type=F32)
            s = jnp.max(s.reshape(dlen // 8, 8, width), axis=0)
            best = jnp.where(wsub == j, jnp.max(s, axis=0, keepdims=True), best)
            if j == 0:
                for item in pending:
                    s_acc = tail(s_acc, *item)
        pending = [(best, [i for _, i in here])]
    (best, ids), = pending
    hi = best.astype(BF16)
    mid = (best - hi.astype(F32)).astype(BF16)
    lo = (best - hi.astype(F32) - mid.astype(F32)).astype(BF16)
    gu = lax.broadcasted_iota(jnp.int32, (lanes, lanes), 0)
    gl = lax.broadcasted_iota(jnp.int32, (lanes, lanes), 1)
    same = gu % nq == gl % nq
    into = jnp.concatenate([jnp.where(same & (gl // nq == i), 1.0, 0.0).astype(BF16) for i in ids], axis=0)
    parts = jnp.dot(jnp.concatenate([hi, mid, lo], axis=0), into, preferred_element_type=F32)
    s_acc = s_acc + (parts[:8] + parts[8:16] + parts[16:24])
    copies[4].wait()
    s_all[me] = s_acc[:ndoc, :] / tbuf[0]

    peers = [(oy, ox, c) for oy in range(ny) for ox in range(nx) for c in range(CORES)][1:]
    peers.sort(key=lambda p: -min(p[0], ny - p[0]) - min(p[1], nx - p[1]))
    for oy, ox, c in peers:
        pltpu.make_async_remote_copy(
            src_ref=s_all.at[me], dst_ref=s_all.at[me],
            send_sem=sems.at[2], recv_sem=sems.at[3],
            device_id=dev(step(y, oy, ny), step(x, ox, nx), step(core, c, CORES)), device_id_type=MESH).start()
    wait_bytes(qt_all, nchip - 1, sems.at[0])
    wait_bytes(qt_all, nchip, sems.at[1])
    wait_bytes(s_all, ndev - 1, sems.at[3])

    logits = s_all[...]
    top = jnp.max(jnp.max(logits, axis=0), axis=0, keepdims=True)
    total = jnp.sum(jnp.sum(jnp.exp(logits - top[None]), axis=0), axis=0, keepdims=True)
    dd = lax.broadcasted_iota(jnp.int32, logits.shape, 0)
    dj = lax.broadcasted_iota(jnp.int32, logits.shape, 1)
    dl = lax.broadcasted_iota(jnp.int32, logits.shape, 2)
    diag = jnp.sum(jnp.sum(jnp.where(dd * nq + dj == dl, logits, 0.0), axis=0), axis=0, keepdims=True)
    losses = top + jnp.log(total) - diag
    nrow = ndev * nq
    home = pltpu.roll(jnp.broadcast_to(losses, (8, nrow)), lax.rem(nrow - me * nq, nrow), 1)
    mean = jnp.sum(losses, axis=1, keepdims=True) / nrow
    out_ref[...] = jnp.where(lax.broadcasted_iota(jnp.int32, home.shape, 0) == 0, home, mean)

    wait_bytes(s_all, ndev - 1, sems.at[2])


def finish(vec_ref, loss_ref, mean_ref):
    loss_ref[...] = vec_ref[0, :loss_ref.shape[0]]
    mean_ref[...] = vec_ref[1, :1]


def solution(mesh):
    ny = mesh.shape["data2"]
    nx = mesh.shape["data"] // CORES
    row_spec = P(("replica", "data2", "data"))
    tok_spec = P(("replica", "data2", "data"), None, None)
    mask_spec = P(("replica", "data2", "data"), None)

    def local_step(query_hidden, doc_hidden, w_proj, query_mask, doc_mask, temperature):
        nq, qlen, hidden = query_hidden.shape
        ndoc, dlen, _ = doc_hidden.shape
        proj = w_proj.shape[1]
        ndev = ny * nx * CORES
        rows, depth = 128, 1
        cfg = (ny, nx, nq, qlen, ndoc, dlen, rows, depth)
        dma = pltpu.SemaphoreType.DMA
        vec = pl.pallas_call(
            functools.partial(kernel, cfg),
            out_shape=pltpu.VMEM((8, ndev * nq), F32),
            in_specs=[pl.BlockSpec(memory_space=pl.ANY)] * 6,
            out_specs=pl.BlockSpec(memory_space=pltpu.VMEM),
            scratch_shapes=[
                pltpu.VMEM((nq * qlen, hidden), BF16),
                pltpu.VMEM((ndoc * dlen, hidden), BF16),
                pltpu.VMEM((hidden, proj), BF16),
                pltpu.VMEM((nq, qlen), jnp.int32),
                pltpu.VMEM((ndoc, dlen), jnp.int32),
                pltpu.VMEM((8, dlen), F32),
                pltpu.SMEM((1,), F32),
                pltpu.VMEM((ndev, proj, nq * qlen), BF16),
                pltpu.VMEM((ndoc * dlen, proj), BF16),
                pltpu.VMEM((dlen, proj), BF16),
                pltpu.VMEM((ndoc, proj, WIDE * nq * qlen), BF16),
                pltpu.VMEM((ndev, ndoc, ndev * nq), F32),
                dma((5,)), dma((ndoc,)), dma((2,)), dma((3,)), dma((4,)),
            ],
            compiler_params=pltpu.CompilerParams(
                collective_id=0, has_side_effects=True, vmem_limit_bytes=60 * 1024 * 1024),
        )(query_hidden.reshape(nq * qlen, hidden), doc_hidden.reshape(ndoc * dlen, hidden),
          w_proj, query_mask, doc_mask, temperature.reshape(1))
        return pl.pallas_call(
            finish,
            out_shape=(jax.ShapeDtypeStruct((nq,), F32), jax.ShapeDtypeStruct((1,), F32)),
            in_specs=[pl.BlockSpec(memory_space=pltpu.VMEM)],
            out_specs=(pl.BlockSpec(memory_space=pltpu.VMEM), pl.BlockSpec(memory_space=pltpu.VMEM)),
            compiler_params=pltpu.CompilerParams(vmem_limit_bytes=1024 * 1024),
        )(vec)

    return jax.shard_map(local_step, mesh=mesh, in_specs=(tok_spec, tok_spec, P(None, None), mask_spec, mask_spec, P()), out_specs=(row_spec, P("replica")), check_vma=False)
```

```python
import functools

import jax
import jax.numpy as jnp
from jax import lax
from jax.experimental import pallas as pl
from jax.experimental.pallas import tpu as pltpu
from jax.sharding import PartitionSpec as P

MESH = pl.DeviceIdType.MESH
F32 = jnp.float32
BF16 = jnp.bfloat16
WIDE = 4
FAR = 1e30
CORES = 2


def offsets(n):
    return sorted(range(1, n), key=lambda o: (min(o, n - o), o))


def kernel(cfg, q_hbm, d_hbm, w_hbm, qm_hbm, dm_hbm, temp_hbm, out_ref,
           qbuf, dbuf, wbuf, qmbuf, dmbuf, dm8, tbuf, qt_all, p_buf, skip, pick, s_all,
           insem, dsem, qrecv, frecv, sems):
    ny, nx, nq, qlen, ndoc, dlen, rows, depth = cfg
    nchip = ny * nx
    ndev = nchip * CORES
    pass_at = 3
    wide = WIDE
    proj = w_hbm.shape[1]
    lanes = nq * qlen
    na, nb = ny, nx
    y = lax.axis_index("data2")
    xc = lax.axis_index("data")
    x = xc // CORES
    core = xc % CORES
    other = 1 - core
    me = (y * nx + x) * CORES + core
    turn = core if ny == nx else 0
    turn_o = other if ny == nx else 0
    a, b = y + turn * (x - y), x + turn * (y - x)
    ao, bo = y + turn_o * (x - y), x + turn_o * (y - x)
    near = [o for o in offsets(na) if min(o, na - o) == 1]
    far = [o for o in offsets(na) if min(o, na - o) > 1]

    def dev(cy, cx, c):
        return {"data2": cy, "data": cx * CORES + c}

    def plane_dev(pa, pb):
        return dev(pa + turn * (pb - pa), pb + turn * (pa - pb), core)

    def step(p, o, n):
        return lax.rem(p + o, n)

    def block(c, i, j):
        c, t, pa, pb = (core, turn, a, b) if c == 0 else (other, turn_o, ao, bo)
        pa, pb = step(pa, i, na), step(pb, j, nb)
        return (c * na + pa) * nb + pb, ((pa + t * (pb - pa)) * nx + pb + t * (pa - pb)) * CORES + c

    def wait_bytes(buf, n, sem):
        pltpu.make_async_copy(buf.at[pl.ds(0, n)], buf.at[pl.ds(0, n)], sem).wait()

    copies = [
        pltpu.make_async_copy(q_hbm, qbuf, insem.at[0]),
        pltpu.make_async_copy(w_hbm, wbuf, insem.at[1]),
        pltpu.make_async_copy(qm_hbm, qmbuf, insem.at[2]),
        pltpu.make_async_copy(dm_hbm, dmbuf, insem.at[3]),
        pltpu.make_async_copy(temp_hbm, tbuf, insem.at[4]),
    ]
    for cp in copies:
        cp.start()

    def doc_copy(j):
        part = pl.ds(j * dlen, dlen)
        return pltpu.make_async_copy(d_hbm.at[part], dbuf.at[part], dsem.at[j])

    for j in range(depth):
        doc_copy(j).start()

    barrier = pltpu.get_barrier_semaphore()
    ring1 = {o: plane_dev(a, step(b, o, nb)) for o in offsets(nb)[::-1]}
    ring2 = {o: plane_dev(step(a, o, na), b) for o in offsets(na)[::-1]}
    partner = dev(y, x, other)
    for d in [*ring2.values(), *ring1.values(), partner]:
        pl.semaphore_signal(barrier, inc=1, device_id=d, device_id_type=MESH)

    copies[2].wait()
    tok_r = lax.broadcasted_iota(jnp.int32, (qlen, lanes), 0)
    tok_l = lax.broadcasted_iota(jnp.int32, (qlen, lanes), 1)
    spread = jnp.where(tok_l // nq == tok_r, 1.0, 0.0).astype(BF16)
    qm = qmbuf[...].astype(F32).astype(BF16)
    qmw = jnp.dot(qm, spread, preferred_element_type=F32)
    qsub = lax.broadcasted_iota(jnp.int32, (nq, lanes), 0)
    qlan = lax.broadcasted_iota(jnp.int32, (nq, lanes), 1)
    qmu = jnp.sum(jnp.where(qlan % nq == qsub, qmw, 0.0), axis=0, keepdims=True)
    pr = lax.broadcasted_iota(jnp.int32, (lanes, lanes), 0)
    pc = lax.broadcasted_iota(jnp.int32, (lanes, lanes), 1)
    perm = jnp.where((pr % qlen) * nq + pr // qlen == pc, qmu, 0.0).astype(BF16)

    def project(block):
        out = jnp.dot(block, wbuf[...], preferred_element_type=F32)
        ss = jnp.sum(out * out, axis=-1, keepdims=True)
        return out * lax.rsqrt(jnp.maximum(ss, 1e-24))

    copies[0].wait()
    copies[1].wait()
    for j in range(depth, min(depth + 1, ndoc)):
        doc_copy(j).start()
    qn = project(qbuf[...]).T.astype(BF16)
    mine = block(0, 0, 0)[0]
    qt_all[mine] = jnp.dot(qn, perm, preferred_element_type=F32).astype(BF16)

    copies[3].wait()
    dm8[...] = jnp.ones_like(dm8)
    dm8[0:ndoc, :] = dmbuf[...].astype(F32)

    pl.semaphore_wait(barrier, na + nb - 1)

    def send(slot, d, send_sem, recv_sem):
        pltpu.make_async_remote_copy(
            src_ref=qt_all.at[slot], dst_ref=qt_all.at[slot], send_sem=send_sem, recv_sem=recv_sem,
            device_id=d, device_id_type=MESH).start()

    cross1 = [(0, o) for o in offsets(nb)]
    cross2 = [(o, 0) for o in offsets(na)]
    rest = [(i, j) for i in near for j in offsets(nb)] + [(i, j) for i in far for j in offsets(nb)]

    def pass_cross():
        wait_bytes(qt_all, len(cross1) + len(cross2) + 1, qrecv.at[0])
        for i, j in cross1:
            for o in near:
                send(block(0, i, j)[0], ring2[o], sems.at[0], qrecv.at[1])
        for i in far:
            for o in offsets(nb):
                send(block(0, i, 0)[0], ring1[o], sems.at[0], qrecv.at[1])
        for i, j in cross1 + cross2:
            send(block(0, i, j)[0], partner, sems.at[0], frecv.at[0])

    def pass_rest():
        wait_bytes(qt_all, len(rest), qrecv.at[1])
        for i, j in rest:
            send(block(0, i, j)[0], partner, sems.at[0], frecv.at[1])

    for d in [*ring2.values(), *ring1.values()]:
        send(mine, d, sems.at[0], qrecv.at[0])
    send(mine, partner, sems.at[0], qrecv.at[0])

    for j in range(depth + 1, ndoc):
        doc_copy(j).start()
    gone = jnp.concatenate([(dm8[...] - 1.0) * FAR, jnp.zeros((proj - 8, dlen), F32)], axis=0)
    skip[...] = gone.T.astype(BF16)
    erow = lax.broadcasted_iota(jnp.int32, pick.shape[1:], 0)
    for j in range(ndoc):
        pick[j] = jnp.where(erow == j, 1.0, 0.0).astype(BF16)

    for j in range(ndoc):
        doc_copy(j).wait()
        if j == pass_at:
            pass_cross()
        for c in range(dlen // rows):
            part = pl.ds(j * dlen + c * rows, rows)
            p_buf[part, :] = project(dbuf[part, :]).astype(BF16)

    lane = lax.broadcasted_iota(jnp.int32, (8, lanes), 1)
    width = wide * lanes
    wsub = lax.broadcasted_iota(jnp.int32, (8, width), 0)

    def tail(s_acc, best, ids):
        for n, i in enumerate(ids):
            v = best[:, n * lanes:(n + 1) * lanes]
            shift = lanes // 2
            while shift >= nq:
                v = v + pltpu.roll(v, shift, 1)
                shift //= 2
            s_acc = jnp.where(lane // nq == i, v, s_acc)
        return s_acc

    arrivals = [
        ([(0, 0, 0)] + [(0, *o) for o in cross1] + [(1, 0, 0)] + [(0, *o) for o in cross2], None),
        ([(1, *o) for o in cross1 + cross2], lambda: wait_bytes(qt_all, len(cross1) + len(cross2), frecv.at[0])),
        ([(0, *o) for o in rest], pass_rest),
        ([(1, *o) for o in rest], lambda: wait_bytes(qt_all, len(rest), frecv.at[1])),
    ]
    queue = [(where, ready if n == 0 else None) for blocks, ready in arrivals for n, where in enumerate(blocks)]

    s_acc = jnp.zeros((8, lanes), F32)
    pending = []
    for g in range(0, len(queue), wide):
        for _, ready in queue[g:g + wide]:
            if ready is not None:
                ready()
        here = [block(*where) for where, _ in queue[g:g + wide]]
        rhs = jnp.concatenate([qt_all[slot] for slot, _ in here], axis=1)
        best = jnp.zeros((8, width), F32)
        for j in range(ndoc):
            s = jnp.dot(jnp.concatenate([p_buf[pl.ds(j * dlen, dlen), :], skip[...]], axis=1),
                        jnp.concatenate([rhs, pick[j]], axis=0), preferred_element_type=F32)
            s = jnp.max(s.reshape(dlen // 8, 8, width), axis=0)
            best = jnp.where(wsub == j, jnp.max(s, axis=0, keepdims=True), best)
            if j == 0:
                for item in pending:
                    s_acc = tail(s_acc, *item)
        pending = [(best, [i for _, i in here])]
    (best, ids), = pending
    hi = best.astype(BF16)
    mid = (best - hi.astype(F32)).astype(BF16)
    lo = (best - hi.astype(F32) - mid.astype(F32)).astype(BF16)
    gu = lax.broadcasted_iota(jnp.int32, (lanes, lanes), 0)
    gl = lax.broadcasted_iota(jnp.int32, (lanes, lanes), 1)
    same = gu % nq == gl % nq
    into = jnp.concatenate([jnp.where(same & (gl // nq == i), 1.0, 0.0).astype(BF16) for i in ids], axis=0)
    parts = jnp.dot(jnp.concatenate([hi, mid, lo], axis=0), into, preferred_element_type=F32)
    s_acc = s_acc + (parts[:8] + parts[8:16] + parts[16:24])
    copies[4].wait()
    s_all[me] = s_acc[:ndoc, :] / tbuf[0]

    peers = [(oy, ox, c) for oy in range(ny) for ox in range(nx) for c in range(CORES)][1:]
    peers.sort(key=lambda p: -min(p[0], ny - p[0]) - min(p[1], nx - p[1]))
    for oy, ox, c in peers:
        pltpu.make_async_remote_copy(
            src_ref=s_all.at[me], dst_ref=s_all.at[me],
            send_sem=sems.at[1], recv_sem=sems.at[2],
            device_id=dev(step(y, oy, ny), step(x, ox, nx), step(core, c, CORES)), device_id_type=MESH).start()
    wait_bytes(qt_all, ndev - 1, sems.at[0])
    wait_bytes(s_all, ndev - 1, sems.at[2])

    logits = s_all[...]
    top = jnp.max(jnp.max(logits, axis=0), axis=0, keepdims=True)
    total = jnp.sum(jnp.sum(jnp.exp(logits - top[None]), axis=0), axis=0, keepdims=True)
    dd = lax.broadcasted_iota(jnp.int32, logits.shape, 0)
    dj = lax.broadcasted_iota(jnp.int32, logits.shape, 1)
    dl = lax.broadcasted_iota(jnp.int32, logits.shape, 2)
    diag = jnp.sum(jnp.sum(jnp.where(dd * nq + dj == dl, logits, 0.0), axis=0), axis=0, keepdims=True)
    losses = top + jnp.log(total) - diag
    nrow = ndev * nq
    home = pltpu.roll(jnp.broadcast_to(losses, (8, nrow)), lax.rem(nrow - me * nq, nrow), 1)
    mean = jnp.sum(losses, axis=1, keepdims=True) / nrow
    out_ref[...] = jnp.where(lax.broadcasted_iota(jnp.int32, home.shape, 0) == 0, home, mean)

    wait_bytes(s_all, ndev - 1, sems.at[1])


def finish(vec_ref, loss_ref, mean_ref):
    loss_ref[...] = vec_ref[0, :loss_ref.shape[0]]
    mean_ref[...] = vec_ref[1, :1]


def solution(mesh):
    ny = mesh.shape["data2"]
    nx = mesh.shape["data"] // CORES
    row_spec = P(("replica", "data2", "data"))
    tok_spec = P(("replica", "data2", "data"), None, None)
    mask_spec = P(("replica", "data2", "data"), None)

    def local_step(query_hidden, doc_hidden, w_proj, query_mask, doc_mask, temperature):
        nq, qlen, hidden = query_hidden.shape
        ndoc, dlen, _ = doc_hidden.shape
        proj = w_proj.shape[1]
        ndev = ny * nx * CORES
        rows, depth = 128, 1
        cfg = (ny, nx, nq, qlen, ndoc, dlen, rows, depth)
        dma = pltpu.SemaphoreType.DMA
        vec = pl.pallas_call(
            functools.partial(kernel, cfg),
            out_shape=pltpu.VMEM((8, ndev * nq), F32),
            in_specs=[pl.BlockSpec(memory_space=pl.ANY)] * 6,
            out_specs=pl.BlockSpec(memory_space=pltpu.VMEM),
            scratch_shapes=[
                pltpu.VMEM((nq * qlen, hidden), BF16),
                pltpu.VMEM((ndoc * dlen, hidden), BF16),
                pltpu.VMEM((hidden, proj), BF16),
                pltpu.VMEM((nq, qlen), jnp.int32),
                pltpu.VMEM((ndoc, dlen), jnp.int32),
                pltpu.VMEM((8, dlen), F32),
                pltpu.SMEM((1,), F32),
                pltpu.VMEM((ndev, proj, nq * qlen), BF16),
                pltpu.VMEM((ndoc * dlen, proj), BF16),
                pltpu.VMEM((dlen, proj), BF16),
                pltpu.VMEM((ndoc, proj, WIDE * nq * qlen), BF16),
                pltpu.VMEM((ndev, ndoc, ndev * nq), F32),
                dma((5,)), dma((ndoc,)), dma((2,)), dma((2,)), dma((3,)),
            ],
            compiler_params=pltpu.CompilerParams(
                collective_id=0, has_side_effects=True, vmem_limit_bytes=60 * 1024 * 1024),
        )(query_hidden.reshape(nq * qlen, hidden), doc_hidden.reshape(ndoc * dlen, hidden),
          w_proj, query_mask, doc_mask, temperature.reshape(1))
        return pl.pallas_call(
            finish,
            out_shape=(jax.ShapeDtypeStruct((nq,), F32), jax.ShapeDtypeStruct((1,), F32)),
            in_specs=[pl.BlockSpec(memory_space=pltpu.VMEM)],
            out_specs=(pl.BlockSpec(memory_space=pltpu.VMEM), pl.BlockSpec(memory_space=pltpu.VMEM)),
            compiler_params=pltpu.CompilerParams(vmem_limit_bytes=1024 * 1024),
        )(vec)

    return jax.shard_map(local_step, mesh=mesh, in_specs=(tok_spec, tok_spec, P(None, None), mask_spec, mask_spec, P()), out_specs=(row_spec, P("replica")), check_vma=False)
```

```python
import functools

import jax
import jax.numpy as jnp
from jax import lax
from jax.experimental import pallas as pl
from jax.experimental.pallas import tpu as pltpu
from jax.sharding import PartitionSpec as P

MESH = pl.DeviceIdType.MESH
F32 = jnp.float32
BF16 = jnp.bfloat16
WIDE = 4
FAR = 1e30
CORES = 2


def offsets(n):
    return sorted(range(1, n), key=lambda o: (min(o, n - o), o))


def kernel(cfg, q_hbm, d_hbm, w_hbm, qm_hbm, dm_hbm, temp_hbm, out_ref,
           qbuf, dbuf, wbuf, qmbuf, dmbuf, dm8, tbuf, qt_all, p_buf, skip, pick, s_all,
           insem, dsem, qrecv, frecv, sems):
    ny, nx, nq, qlen, ndoc, dlen, rows, depth = cfg
    nchip = ny * nx
    ndev = nchip * CORES
    pass_at = 3
    wide = WIDE
    proj = w_hbm.shape[1]
    lanes = nq * qlen
    na, nb = ny, nx
    y = lax.axis_index("data2")
    xc = lax.axis_index("data")
    x = xc // CORES
    core = xc % CORES
    other = 1 - core
    me = (y * nx + x) * CORES + core
    turn = core if ny == nx else 0
    turn_o = other if ny == nx else 0
    a, b = y + turn * (x - y), x + turn * (y - x)
    ao, bo = y + turn_o * (x - y), x + turn_o * (y - x)
    near = [o for o in offsets(na) if min(o, na - o) == 1]
    far = [o for o in offsets(na) if min(o, na - o) > 1]

    def dev(cy, cx, c):
        return {"data2": cy, "data": cx * CORES + c}

    def plane_dev(pa, pb):
        return dev(pa + turn * (pb - pa), pb + turn * (pa - pb), core)

    def step(p, o, n):
        return lax.rem(p + o, n)

    def block(c, i, j):
        c, t, pa, pb = (core, turn, a, b) if c == 0 else (other, turn_o, ao, bo)
        pa, pb = step(pa, i, na), step(pb, j, nb)
        return (c * na + pa) * nb + pb, ((pa + t * (pb - pa)) * nx + pb + t * (pa - pb)) * CORES + c

    def wait_bytes(buf, n, sem):
        pltpu.make_async_copy(buf.at[pl.ds(0, n)], buf.at[pl.ds(0, n)], sem).wait()

    copies = [
        pltpu.make_async_copy(q_hbm, qbuf, insem.at[0]),
        pltpu.make_async_copy(w_hbm, wbuf, insem.at[1]),
        pltpu.make_async_copy(qm_hbm, qmbuf, insem.at[2]),
        pltpu.make_async_copy(dm_hbm, dmbuf, insem.at[3]),
        pltpu.make_async_copy(temp_hbm, tbuf, insem.at[4]),
    ]
    for cp in copies:
        cp.start()

    def doc_copy(j):
        part = pl.ds(j * dlen, dlen)
        return pltpu.make_async_copy(d_hbm.at[part], dbuf.at[part], dsem.at[j])

    for j in range(depth):
        doc_copy(j).start()

    barrier = pltpu.get_barrier_semaphore()
    ring1 = {o: plane_dev(a, step(b, o, nb)) for o in offsets(nb)[::-1]}
    ring2 = {o: plane_dev(step(a, o, na), b) for o in offsets(na)[::-1]}
    partner = dev(y, x, other)
    for d in [*ring2.values(), *ring1.values(), partner]:
        pl.semaphore_signal(barrier, inc=1, device_id=d, device_id_type=MESH)

    copies[2].wait()
    tok_r = lax.broadcasted_iota(jnp.int32, (qlen, lanes), 0)
    tok_l = lax.broadcasted_iota(jnp.int32, (qlen, lanes), 1)
    spread = jnp.where(tok_l // nq == tok_r, 1.0, 0.0).astype(BF16)
    qm = qmbuf[...].astype(F32).astype(BF16)
    qmw = jnp.dot(qm, spread, preferred_element_type=F32)
    qsub = lax.broadcasted_iota(jnp.int32, (nq, lanes), 0)
    qlan = lax.broadcasted_iota(jnp.int32, (nq, lanes), 1)
    qmu = jnp.sum(jnp.where(qlan % nq == qsub, qmw, 0.0), axis=0, keepdims=True)
    pr = lax.broadcasted_iota(jnp.int32, (lanes, lanes), 0)
    pc = lax.broadcasted_iota(jnp.int32, (lanes, lanes), 1)
    perm = jnp.where((pr % qlen) * nq + pr // qlen == pc, qmu, 0.0).astype(BF16)

    def project(block):
        out = jnp.dot(block, wbuf[...], preferred_element_type=F32)
        ss = jnp.sum(out * out, axis=-1, keepdims=True)
        return out * lax.rsqrt(jnp.maximum(ss, 1e-24))

    copies[0].wait()
    copies[1].wait()
    for j in range(depth, min(depth + 1, ndoc)):
        doc_copy(j).start()
    qn = project(qbuf[...]).T.astype(BF16)
    mine = block(0, 0, 0)[0]
    qt_all[mine] = jnp.dot(qn, perm, preferred_element_type=F32).astype(BF16)

    copies[3].wait()
    dm8[...] = jnp.ones_like(dm8)
    dm8[0:ndoc, :] = dmbuf[...].astype(F32)

    pl.semaphore_wait(barrier, na + nb - 1)

    def send(slot, d, send_sem, recv_sem):
        pltpu.make_async_remote_copy(
            src_ref=qt_all.at[slot], dst_ref=qt_all.at[slot], send_sem=send_sem, recv_sem=recv_sem,
            device_id=d, device_id_type=MESH).start()

    cross1 = [(0, o) for o in offsets(nb)]
    cross2 = [(o, 0) for o in offsets(na)]
    rest = [(i, j) for i in near for j in offsets(nb)] + [(i, j) for i in far for j in offsets(nb)]

    def pass_cross():
        wait_bytes(qt_all, len(cross1) + len(cross2) + 1, qrecv.at[0])
        for i, j in cross1:
            for o in near:
                send(block(0, i, j)[0], ring2[o], sems.at[0], qrecv.at[1])
        for i in far:
            for o in offsets(nb):
                send(block(0, i, 0)[0], ring1[o], sems.at[0], qrecv.at[1])
        for i, j in cross1 + cross2:
            send(block(0, i, j)[0], partner, sems.at[0], frecv.at[0])

    def pass_rest():
        wait_bytes(qt_all, len(rest), qrecv.at[1])
        for i, j in rest:
            send(block(0, i, j)[0], partner, sems.at[0], frecv.at[1])

    for d in [*ring2.values(), *ring1.values()]:
        send(mine, d, sems.at[0], qrecv.at[0])
    send(mine, partner, sems.at[0], qrecv.at[0])

    for j in range(depth + 1, ndoc):
        doc_copy(j).start()
    gone = jnp.concatenate([(dm8[...] - 1.0) * FAR, jnp.zeros((proj - 8, dlen), F32)], axis=0)
    skip[...] = gone.T.astype(BF16)
    erow = lax.broadcasted_iota(jnp.int32, pick.shape[1:], 0)
    for j in range(ndoc):
        pick[j] = jnp.where(erow == j, 1.0, 0.0).astype(BF16)

    for j in range(ndoc):
        doc_copy(j).wait()
        if j == pass_at:
            pass_cross()
        for c in range(dlen // rows):
            part = pl.ds(j * dlen + c * rows, rows)
            p_buf[part, :] = project(dbuf[part, :]).astype(BF16)

    lane = lax.broadcasted_iota(jnp.int32, (8, lanes), 1)
    width = wide * lanes
    wsub = lax.broadcasted_iota(jnp.int32, (8, width), 0)

    def tail(s_acc, best, ids):
        for n, i in enumerate(ids):
            v = best[:, n * lanes:(n + 1) * lanes]
            shift = lanes // 2
            while shift >= nq:
                v = v + pltpu.roll(v, shift, 1)
                shift //= 2
            s_acc = jnp.where(lane // nq == i, v, s_acc)
        return s_acc

    arrivals = [
        ([(0, 0, 0)] + [(0, *o) for o in cross1] + [(1, 0, 0)] + [(0, *o) for o in cross2], None),
        ([(1, *o) for o in cross1 + cross2], lambda: wait_bytes(qt_all, len(cross1) + len(cross2), frecv.at[0])),
        ([(0, *o) for o in rest], pass_rest),
        ([(1, *o) for o in rest], lambda: wait_bytes(qt_all, len(rest), frecv.at[1])),
    ]
    queue = [(where, ready if n == 0 else None) for blocks, ready in arrivals for n, where in enumerate(blocks)]

    s_acc = jnp.zeros((8, lanes), F32)
    pending = []
    for g in range(0, len(queue), wide):
        for _, ready in queue[g:g + wide]:
            if ready is not None:
                ready()
        here = [block(*where) for where, _ in queue[g:g + wide]]
        rhs = jnp.concatenate([qt_all[slot] for slot, _ in here], axis=1)
        best = jnp.zeros((8, width), F32)
        for j in range(ndoc):
            s = jnp.dot(jnp.concatenate([p_buf[pl.ds(j * dlen, dlen), :], skip[...]], axis=1),
                        jnp.concatenate([rhs, pick[j]], axis=0), preferred_element_type=F32)
            s = jnp.max(s.reshape(dlen // 8, 8, width), axis=0)
            best = jnp.where(wsub == j, jnp.max(s, axis=0, keepdims=True), best)
            if j == 0:
                for item in pending:
                    s_acc = tail(s_acc, *item)
        pending = [(best, [i for _, i in here])]
    (best, ids), = pending
    hi = best.astype(BF16)
    mid = (best - hi.astype(F32)).astype(BF16)
    lo = (best - hi.astype(F32) - mid.astype(F32)).astype(BF16)
    gu = lax.broadcasted_iota(jnp.int32, (lanes, lanes), 0)
    gl = lax.broadcasted_iota(jnp.int32, (lanes, lanes), 1)
    same = gu % nq == gl % nq
    into = jnp.concatenate([jnp.where(same & (gl // nq == i), 1.0, 0.0).astype(BF16) for i in ids], axis=0)
    parts = jnp.dot(jnp.concatenate([hi, mid, lo], axis=0), into, preferred_element_type=F32)
    s_acc = s_acc + (parts[:8] + parts[8:16] + parts[16:24])
    copies[4].wait()
    s_all[me] = s_acc[:ndoc, :] / tbuf[0]

    peers = [(oy, ox, c) for oy in range(ny) for ox in range(nx) for c in range(CORES)][1:]
    peers.sort(key=lambda p: {3: 0, 4: 1, 2: 2, 1: 3, 0: 4}[min(p[0], ny - p[0]) + min(p[1], nx - p[1])])
    for oy, ox, c in peers:
        pltpu.make_async_remote_copy(
            src_ref=s_all.at[me], dst_ref=s_all.at[me],
            send_sem=sems.at[1], recv_sem=sems.at[2],
            device_id=dev(step(y, oy, ny), step(x, ox, nx), step(core, c, CORES)), device_id_type=MESH).start()
    wait_bytes(qt_all, ndev - 1, sems.at[0])
    wait_bytes(s_all, ndev - 1, sems.at[2])

    logits = s_all[...]
    top = jnp.max(jnp.max(logits, axis=0), axis=0, keepdims=True)
    total = jnp.sum(jnp.sum(jnp.exp(logits - top[None]), axis=0), axis=0, keepdims=True)
    dd = lax.broadcasted_iota(jnp.int32, logits.shape, 0)
    dj = lax.broadcasted_iota(jnp.int32, logits.shape, 1)
    dl = lax.broadcasted_iota(jnp.int32, logits.shape, 2)
    diag = jnp.sum(jnp.sum(jnp.where(dd * nq + dj == dl, logits, 0.0), axis=0), axis=0, keepdims=True)
    losses = top + jnp.log(total) - diag
    nrow = ndev * nq
    home = pltpu.roll(jnp.broadcast_to(losses, (8, nrow)), lax.rem(nrow - me * nq, nrow), 1)
    mean = jnp.sum(losses, axis=1, keepdims=True) / nrow
    out_ref[...] = jnp.where(lax.broadcasted_iota(jnp.int32, home.shape, 0) == 0, home, mean)

    wait_bytes(s_all, ndev - 1, sems.at[1])


def finish(vec_ref, loss_ref, mean_ref):
    loss_ref[...] = vec_ref[0, :loss_ref.shape[0]]
    mean_ref[...] = vec_ref[1, :1]


def solution(mesh):
    ny = mesh.shape["data2"]
    nx = mesh.shape["data"] // CORES
    row_spec = P(("replica", "data2", "data"))
    tok_spec = P(("replica", "data2", "data"), None, None)
    mask_spec = P(("replica", "data2", "data"), None)

    def local_step(query_hidden, doc_hidden, w_proj, query_mask, doc_mask, temperature):
        nq, qlen, hidden = query_hidden.shape
        ndoc, dlen, _ = doc_hidden.shape
        proj = w_proj.shape[1]
        ndev = ny * nx * CORES
        rows, depth = 128, 1
        cfg = (ny, nx, nq, qlen, ndoc, dlen, rows, depth)
        dma = pltpu.SemaphoreType.DMA
        vec = pl.pallas_call(
            functools.partial(kernel, cfg),
            out_shape=pltpu.VMEM((8, ndev * nq), F32),
            in_specs=[pl.BlockSpec(memory_space=pl.ANY)] * 6,
            out_specs=pl.BlockSpec(memory_space=pltpu.VMEM),
            scratch_shapes=[
                pltpu.VMEM((nq * qlen, hidden), BF16),
                pltpu.VMEM((ndoc * dlen, hidden), BF16),
                pltpu.VMEM((hidden, proj), BF16),
                pltpu.VMEM((nq, qlen), jnp.int32),
                pltpu.VMEM((ndoc, dlen), jnp.int32),
                pltpu.VMEM((8, dlen), F32),
                pltpu.SMEM((1,), F32),
                pltpu.VMEM((ndev, proj, nq * qlen), BF16),
                pltpu.VMEM((ndoc * dlen, proj), BF16),
                pltpu.VMEM((dlen, proj), BF16),
                pltpu.VMEM((ndoc, proj, WIDE * nq * qlen), BF16),
                pltpu.VMEM((ndev, ndoc, ndev * nq), F32),
                dma((5,)), dma((ndoc,)), dma((2,)), dma((2,)), dma((3,)),
            ],
            compiler_params=pltpu.CompilerParams(
                collective_id=0, has_side_effects=True, vmem_limit_bytes=60 * 1024 * 1024),
        )(query_hidden.reshape(nq * qlen, hidden), doc_hidden.reshape(ndoc * dlen, hidden),
          w_proj, query_mask, doc_mask, temperature.reshape(1))
        return pl.pallas_call(
            finish,
            out_shape=(jax.ShapeDtypeStruct((nq,), F32), jax.ShapeDtypeStruct((1,), F32)),
            in_specs=[pl.BlockSpec(memory_space=pltpu.VMEM)],
            out_specs=(pl.BlockSpec(memory_space=pltpu.VMEM), pl.BlockSpec(memory_space=pltpu.VMEM)),
            compiler_params=pltpu.CompilerParams(vmem_limit_bytes=1024 * 1024),
        )(vec)

    return jax.shard_map(local_step, mesh=mesh, in_specs=(tok_spec, tok_spec, P(None, None), mask_spec, mask_spec, P()), out_specs=(row_spec, P("replica")), check_vma=False)
```
